32 devices in a mesh: rep: 2 (over z, core), dp: 16 (over x, y).
Axes of the slice: x: 4, y: 4, z: 1, core: 2. Of those that a mesh axis runs over, the one named last changes fastest.
The devices are a block of a 4x4x8 slice.
Arguments:
- g_w_gate: bfloat16 [32, 2, 1024, 4096], P(('rep', 'dp')), parts along dimension 0
- g_w_up: bfloat16 [32, 2, 1024, 4096], P(('rep', 'dp')), parts along dimension 0
- g_w_down: bfloat16 [32, 2, 4096, 1024], P(('rep', 'dp')), parts along dimension 0
- w_gate: bfloat16 [2, 1024, 4096], replicated
- w_up: bfloat16 [2, 1024, 4096], replicated
- w_down: bfloat16 [2, 4096, 1024], replicated
- m_w_gate: float32 [2, 1024, 4096], P(None, 'dp')
- m_w_up: float32 [2, 1024, 4096], P(None, 'dp')
- m_w_down: float32 [2, 4096, 1024], P(None, 'dp')
- v_w_gate: float32 [2, 1024, 4096], P(None, 'dp')
- v_w_up: float32 [2, 1024, 4096], P(None, 'dp')
- v_w_down: float32 [2, 4096, 1024], P(None, 'dp')
Outputs:
- output 1: bfloat16 [4, 1024, 4096], P('rep'), parts along dimension 0
- output 2: bfloat16 [4, 1024, 4096], P('rep'), parts along dimension 0
- output 3: bfloat16 [4, 4096, 1024], P('rep'), parts along dimension 0
- output 4: float32 [4, 1024, 4096], P('rep', 'dp'), parts along dimension 0
- output 5: float32 [4, 1024, 4096], P('rep', 'dp'), parts along dimension 0
- output 6: float32 [4, 4096, 1024], P('rep', 'dp'), parts along dimension 0
- output 7: float32 [4, 1024, 4096], P('rep', 'dp'), parts along dimension 0
- output 8: float32 [4, 1024, 4096], P('rep', 'dp'), parts along dimension 0
- output 9: float32 [4, 4096, 1024], P('rep', 'dp'), parts along dimension 0
There are 2 independent parts. The reference program is written for one: setup_inputs(seed, part) draws one part's arguments, and reference() takes and returns one part's arrays. A program takes and returns all parts, laid end to end along the dimension named above; an argument that names none is the same for every part.
All inputs are finite; a program needn't handle non-finite values.
Results may differ from the reference program's by a relative error of at most 0.022.
Values are sent between devices in bfloat16 or wider.
A program may use at most 768 MiB of HBM per device.

```python
import jax
import jax.numpy as jnp
from jax import lax

DEVICES = 16
D = 1024
FF = 4096
LAYERS = 2
NAMES = ("w_gate", "w_up", "w_down")
SHAPES = {"w_gate": (LAYERS, D, FF), "w_up": (LAYERS, D, FF), "w_down": (LAYERS, FF, D)}


def setup_inputs(seed: int = 0, part: int = 0) -> dict:
    kz, *keys = jax.random.split(jax.random.key(seed), 1 + 5 * len(NAMES))
    loud = 2.0 ** jax.random.uniform(kz, (), jnp.float32, -1.0, 1.0)
    drawn = {}
    for name, key, both in zip(NAMES, keys[:3], keys[3:6], strict=True):
        own = jax.random.normal(jax.random.fold_in(key, part), (DEVICES, *SHAPES[name]), jnp.float32)
        shared = jax.random.normal(jax.random.fold_in(both, part), SHAPES[name], jnp.float32)
        drawn["g_" + name] = (loud * (0.7 * shared / DEVICES + 0.7 * own * DEVICES**-0.5)).astype(jnp.bfloat16)
    for name, key in zip(NAMES, keys[6:9], strict=True):
        drawn[name] = (jax.random.normal(key, SHAPES[name], jnp.float32) * SHAPES[name][1] ** -0.5).astype(jnp.bfloat16)
    for name, key in zip(NAMES, keys[9:12], strict=True):
        drawn["m_" + name] = loud * 0.5 * jax.random.normal(key, SHAPES[name], jnp.float32)
    for name, key in zip(NAMES, keys[12:15], strict=True):
        drawn["v_" + name] = loud * loud * jax.random.uniform(key, SHAPES[name], jnp.float32, 0.5, 1.5)
    return drawn


def adamw(w, m, v, g):
    m = 0.9 * m + 0.1 * g
    v = 0.95 * v + 0.05 * g * g
    step = m * lax.rsqrt(v + 1e-8) + 0.1 * w
    return (w - 0.02 * step).astype(jnp.bfloat16), m, v


def reference(g_w_gate, g_w_up, g_w_down, w_gate, w_up, w_down, m_w_gate, m_w_up, m_w_down, v_w_gate, v_w_up, v_w_down):
    def total(terms):
        return lax.scan(lambda so_far, term: (so_far + term.astype(jnp.float32), None), jnp.zeros(terms.shape[1:], jnp.float32), terms)[0]

    gradients = [total(terms).astype(jnp.bfloat16).astype(jnp.float32) for terms in (g_w_gate, g_w_up, g_w_down)]
    new = [
        adamw(w.astype(jnp.float32), m, v, g)
        for w, m, v, g in zip((w_gate, w_up, w_down), (m_w_gate, m_w_up, m_w_down), (v_w_gate, v_w_up, v_w_down), gradients, strict=True)
    ]
    return tuple(one[which] for which in range(3) for one in new)
```

```python
import functools
import math

import jax
import jax.numpy as jnp
from jax import lax
from jax.experimental import pallas as pl
from jax.experimental.pallas import tpu as pltpu
from jax.sharding import PartitionSpec as P

MESH = pl.DeviceIdType.MESH
F32, BF16 = jnp.float32, jnp.bfloat16
STAGES = 9


def adamw(w, m, v, g):
    m = 0.9 * m + 0.1 * g
    v = 0.95 * v + 0.05 * g * g
    step = m * lax.rsqrt(v + 1e-8) + 0.1 * w
    return (w - 0.02 * step).astype(BF16), m, v


def step_kernel(side, piece, per_weight, *refs):
    n_w = 3
    grads, weights, ms, vs = (refs[i * n_w : (i + 1) * n_w] for i in range(4))
    wholes, new_ms, new_vs = (refs[i * n_w : (i + 1) * n_w] for i in range(4, 7))
    (l1, l2, m1, m2, o1, o2, w_in, m_io, v_io, kept, kept_half, w_new,
     send_sem, r_sem, ag_sem, o1_sem, o2_sem, in_sem, out_sem, own_sem) = refs[7 * n_w :]
    rows, cols = piece
    half = cols // 2
    chunks = n_w * per_weight
    me = lax.axis_index("dp")
    x, y = me // side, me % side

    def at(px, py):
        return {"dp": px * side + py}

    xs = [(x + 1) % side, (x + side - 1) % side]
    ys = [(y + 1) % side, (y + side - 1) % side]
    along_x, along_y = [at(i, y) for i in xs], [at(x, i) for i in ys]

    barrier = pltpu.get_barrier_semaphore()
    for device in along_x + along_y:
        pl.semaphore_signal(barrier, inc=1, device_id=device, device_id_type=MESH)
    pl.semaphore_wait(barrier, 4)

    layers = [
        dict(l=0, p=x, q=y, ps=xs, qs=ys, first=along_x, second=along_y),
        dict(l=1, p=y, q=x, ps=ys, qs=xs, first=along_y, second=along_x),
    ]

    def region(ref, k, part=None):
        if ref.shape[-2] == rows:
            row, col = pl.ds(0, rows), k * cols
        else:
            row, col = pl.ds(pl.multiple_of(k * rows, rows), rows), 0
        if part is None:
            return row, pl.ds(pl.multiple_of(col, cols) if not isinstance(col, int) else col, cols)
        col = col + part * half
        return row, pl.ds(pl.multiple_of(col, half) if not isinstance(col, int) else col, half)

    def block(ref, L, p, q, k, part=None):
        row, col = region(ref, k, part)
        return ref.at[(L["l"], p, q, row, col) if L["l"] == 0 else (L["l"], q, p, row, col)]

    def mine(ref, L, k):
        return ref.at[(L["l"], *region(ref, k))]

    def part_of(ref, part):
        return ref.at[..., pl.ds(part * half, half)]

    def for_weight(c, fn):
        for i in range(n_w):
            pl.when(c // per_weight == i)(functools.partial(fn, i, c % per_weight))

    def send(src, dst, s_sem, d_sem, device):
        pltpu.make_async_remote_copy(src, dst, s_sem, d_sem, device_id=device, device_id_type=MESH).start()

    def wait(ref, sem):
        pltpu.make_async_copy(ref, ref, sem).wait()

    every = pl.ds(0, side)

    def stage1(L, c):
        l = L["l"]

        def go(i, k):
            far = (L["p"] + 2) % side
            for d in range(2):
                send(block(grads[i], L, far, every, k, 1 - d), l1.at[c, l, d], send_sem.at[c, l, 0], r_sem.at[c, l, 0], L["first"][d])
            for d in range(2):
                send(block(grads[i], L, L["ps"][d], every, k, d), part_of(l2.at[c, l, d], d), send_sem.at[c, l, 0], r_sem.at[c, l, 1], L["first"][d])
                pltpu.make_async_copy(block(grads[i], L, L["ps"][d], every, k, 1 - d), o1.at[c % 2, l, d], o1_sem.at[c % 2, l, d]).start()

        for_weight(c, go)

    def stage2(L, c):
        l = L["l"]
        for_weight(c, lambda i, k: pltpu.make_async_copy(block(grads[i], L, L["p"], every, k), o2.at[c % 2, l], o2_sem.at[c % 2, l]).start())
        wait(l1.at[c, l], r_sem.at[c, l, 0])
        for d in range(2):
            wait(o1.at[c % 2, l, d], o1_sem.at[c % 2, l, d])

            @pl.loop(0, side * (rows // 16))
            def _(j):
                b, r = j // (rows // 16), pl.ds(pl.multiple_of(j % (rows // 16) * 16, 16), 16)
                l1[c, l, d, b, r, :] = (l1[c, l, d, b, r, :].astype(F32) + o1[c % 2, l, d, b, r, :].astype(F32)).astype(BF16)

            send(l1.at[c, l, d], part_of(l2.at[c, l, d], 1 - d), send_sem.at[c, l, 0], r_sem.at[c, l, 1], L["first"][d])

    def stage3(L, c):
        l, q = L["l"], L["q"]
        wait(l2.at[c, l], r_sem.at[c, l, 1])
        wait(o2.at[c % 2, l], o2_sem.at[c % 2, l])
        low, high = pl.ds(0, half), pl.ds(half, half)

        def total(b, r, col):
            return l2[c, l, 0, b, r, col].astype(F32) + l2[c, l, 1, b, r, col].astype(F32) + o2[c % 2, l, b, r, col].astype(F32)

        far = (q + 2) % side

        @pl.loop(0, rows // 16)
        def _(j):
            r = pl.ds(pl.multiple_of(j * 16, 16), 16)
            for col in (low, high):
                kept[c % 3, l, r, col] = total(q, r, col)
                l2[c, l, 0, far, r, col] = total(far, r, col).astype(BF16)
            for d, (direct, later) in enumerate(((low, high), (high, low))):
                near = L["qs"][d]
                kept_half[c % 3, l, d, r, :] = total(near, r, later)
                l2[c, l, 0, near, r, direct] = total(near, r, direct).astype(BF16)

        for d in range(2):
            send(part_of(l2.at[c, l, 0, far], 1 - d), m1.at[c, l, d], send_sem.at[c, l, 1], r_sem.at[c, l, 2], L["second"][d])
        for d in range(2):
            send(part_of(l2.at[c, l, 0, L["qs"][d]], d), part_of(m2.at[c, l, d], d), send_sem.at[c, l, 1], r_sem.at[c, l, 3], L["second"][d])

    def stage4(L, c):
        l = L["l"]

        def load(i, k):
            for ref, buffer, s in (
                (block(weights[i], L, L["p"], L["q"], k), w_in, 0),
                (mine(ms[i], L, k), m_io, 1),
                (mine(vs[i], L, k), v_io, 2),
            ):
                pltpu.make_async_copy(ref, buffer.at[c % 2, l], in_sem.at[c % 2, l, s]).start()

        @pl.when(c >= 2)
        def _():
            wait(m_io.at[c % 2, l], out_sem.at[c % 2, l, 0])
            wait(v_io.at[c % 2, l], out_sem.at[c % 2, l, 1])

        for_weight(c, load)
        wait(m1.at[c, l], r_sem.at[c, l, 2])
        for d in range(2):

            @pl.loop(0, rows // 16)
            def _(j):
                r = pl.ds(pl.multiple_of(j * 16, 16), 16)
                m1[c, l, d, r, :] = (m1[c, l, d, r, :].astype(F32) + kept_half[c % 3, l, d, r, :]).astype(BF16)

            send(m1.at[c, l, d], part_of(m2.at[c, l, d], 1 - d), send_sem.at[c, l, 1], r_sem.at[c, l, 3], L["second"][d])

    def stage5(L, c):
        l = L["l"]
        wait(m2.at[c, l], r_sem.at[c, l, 3])
        for s, buffer in enumerate((w_in, m_io, v_io)):
            wait(buffer.at[c % 2, l], in_sem.at[c % 2, l, s])

        @pl.loop(0, rows // 16)
        def _(j):
            r = pl.ds(pl.multiple_of(j * 16, 16), 16)
            g = kept[c % 3, l, r, :] + m2[c, l, 0, r, :].astype(F32) + m2[c, l, 1, r, :].astype(F32)
            g = g.astype(BF16).astype(F32)
            w_new[c, l, r, :], m_io[c % 2, l, r, :], v_io[c % 2, l, r, :] = adamw(
                w_in[c % 2, l, r, :].astype(F32), m_io[c % 2, l, r, :], v_io[c % 2, l, r, :], g
            )

        def go(i, k):
            there = block(wholes[i], L, L["p"], L["q"], k)
            for d in range(2):
                send(w_new.at[c, l], there, send_sem.at[c, l, 2], ag_sem.at[c, l, d], L["second"][d])
            pltpu.make_async_copy(w_new.at[c, l], there, own_sem.at[c % 3, l]).start()
            pltpu.make_async_copy(m_io.at[c % 2, l], mine(new_ms[i], L, k), out_sem.at[c % 2, l, 0]).start()
            pltpu.make_async_copy(v_io.at[c % 2, l], mine(new_vs[i], L, k), out_sem.at[c % 2, l, 1]).start()

        for_weight(c, go)

    def stage6(L, c):
        l = L["l"]

        def go(i, k):
            for d in range(2):
                wait(w_new.at[c, l], ag_sem.at[c, l, d])
                there = block(wholes[i], L, L["p"], L["qs"][1 - d], k, 1 - d)
                send(there, there, send_sem.at[c, l, 2], ag_sem.at[c, l, 2 + d], L["second"][d])

        for_weight(c, go)

    def stage7(L, c):
        l = L["l"]
        wait(w_new.at[c, l], own_sem.at[c % 3, l])
        for d in range(2):
            wait(part_of(w_new.at[c, l], d), ag_sem.at[c, l, 2 + d])

        def go(i, k):
            there = block(wholes[i], L, L["p"], every, k)
            for d in range(2):
                send(there, there, send_sem.at[c, l, 3], ag_sem.at[c, l, 4 + d], L["first"][d])

        for_weight(c, go)

    def stage8(L, c):
        l = L["l"]

        def go(i, k):
            for d in range(2):
                wait(o2.at[0, 0], ag_sem.at[c, l, 4 + d])
                there = block(wholes[i], L, L["ps"][1 - d], every, k, 1 - d)
                send(there, there, send_sem.at[c, l, 3], ag_sem.at[c, l, 6 + d], L["first"][d])

        for_weight(c, go)

    def stage9(L, c):
        l = L["l"]
        for d in range(2):
            wait(o1.at[0, 0, 0], ag_sem.at[c, l, 6 + d])

    stages = (stage1, stage2, stage3, stage4, stage5, stage6, stage7, stage8, stage9)

    @pl.loop(0, chunks + STAGES - 1)
    def _(t):
        for s, stage in enumerate(stages):
            c = t - s

            @pl.when((c >= 0) & (c < chunks))
            def _():
                for L in layers:
                    stage(L, c)

    for L in layers:
        for c in (chunks - 2, chunks - 1):
            wait(m_io.at[c % 2, L["l"]], out_sem.at[c % 2, L["l"], 0])
            wait(v_io.at[c % 2, L["l"]], out_sem.at[c % 2, L["l"], 1])

    three, row, col = pl.ds(0, 3), pl.ds(0, rows), pl.ds(0, cols)

    @pl.loop(0, chunks)
    def _(c):
        for l in range(2):
            wait(wholes[0].at[l, three, every, row, col], send_sem.at[c, l, 0])
            wait(wholes[0].at[l, 0, three, row, col], send_sem.at[c, l, 1])
            wait(wholes[0].at[l, 0, three, row, col], send_sem.at[c, l, 2])
            wait(wholes[0].at[l, three, every, row, col], send_sem.at[c, l, 3])


def solution(mesh):
    n = mesh.shape["dp"]
    side = math.isqrt(n)

    def step(*arrays):
        terms, weights, m, v = (arrays[i : i + 3] for i in (0, 3, 6, 9))
        layers = m[0].shape[0]
        piece = tuple(min(one.shape[i] for one in m) for i in (1, 2))
        rows, cols = piece
        sizes = {one.shape[1] * one.shape[2] for one in m}
        assert side * side == n and side == 4 and layers == 2 and len(sizes) == 1
        per_weight = sizes.pop() // (rows * cols)
        chunks = 3 * per_weight

        def blocks(a, one):
            return a.reshape(layers, side, side, *one.shape[1:])

        inputs = [blocks(a, one) for a, one in zip(terms, m)] + [blocks(a, one) for a, one in zip(weights, m)] + [*m, *v]
        outs = [jax.ShapeDtypeStruct((layers, side, side, *one.shape[1:]), BF16) for one in m]
        outs += [jax.ShapeDtypeStruct(one.shape, F32) for one in (*m, *v)]
        half = cols // 2
        dma = pltpu.SemaphoreType.DMA
        any_space = pl.BlockSpec(memory_space=pl.ANY)
        results = pl.pallas_call(
            functools.partial(step_kernel, side, piece, per_weight),
            out_shape=outs,
            in_specs=[any_space] * 12,
            out_specs=[any_space] * 9,
            scratch_shapes=[
                pltpu.VMEM((chunks, layers, 2, side, rows, half), BF16),
                pltpu.VMEM((chunks, layers, 2, side, rows, cols), BF16),
                pltpu.VMEM((chunks, layers, 2, rows, half), BF16),
                pltpu.VMEM((chunks, layers, 2, rows, cols), BF16),
                pltpu.VMEM((2, layers, 2, side, rows, half), BF16),
                pltpu.VMEM((2, layers, side, rows, cols), BF16),
                pltpu.VMEM((2, layers, rows, cols), BF16),
                pltpu.VMEM((2, layers, rows, cols), F32),
                pltpu.VMEM((2, layers, rows, cols), F32),
                pltpu.VMEM((3, layers, rows, cols), F32),
                pltpu.VMEM((3, layers, 2, rows, half), F32),
                pltpu.VMEM((chunks, layers, rows, cols), BF16),
                dma((chunks, layers, 4)),
                dma((chunks, layers, 4)),
                dma((chunks, layers, 8)),
                dma((2, layers, 2)),
                dma((2, layers)),
                dma((2, layers, 3)),
                dma((2, layers, 2)),
                dma((3, layers)),
            ],
            compiler_params=pltpu.CompilerParams(collective_id=0, has_side_effects=True, vmem_limit_bytes=63 * 2**20),
            name="step",
        )(*inputs)
        whole = [r.reshape(a.shape) for r, a in zip(results[:3], weights)]
        return (*whole, *results[3:])

    all_of, cut = P(None, None, None), P(None, "dp", None)
    return jax.shard_map(
        step,
        mesh=mesh,
        in_specs=(P(("rep", "dp"), None, None, None),) * 3 + (all_of,) * 3 + (cut,) * 6,
        out_specs=(P("rep", None, None),) * 3 + (P("rep", "dp", None),) * 6,
        check_vma=False,
    )
```

```python
import functools
import math

import jax
import jax.numpy as jnp
from jax import lax
from jax.experimental import pallas as pl
from jax.experimental.pallas import tpu as pltpu
from jax.sharding import PartitionSpec as P

MESH = pl.DeviceIdType.MESH
F32, BF16 = jnp.float32, jnp.bfloat16
STAGES = 9
TAIL = 6


def adamw(w, m, v, g):
    m = 0.9 * m + 0.1 * g
    v = 0.95 * v + 0.05 * g * g
    step = m * lax.rsqrt(v + 1e-8) + 0.1 * w
    return (w - 0.02 * step).astype(BF16), m, v


def aligned(start, size):
    return pl.ds(start if isinstance(start, int) else pl.multiple_of(start, size), size)


def region(piece, ref, k, part=None):
    rows, cols = piece
    row, col = (0, k * cols) if ref.shape[-2] == rows else (k * rows, 0)
    if part is None:
        return aligned(row, rows), aligned(col, cols)
    return aligned(row, rows), aligned(col + part * (cols // 2), cols // 2)


def block_of(piece, ref, L, p, q, k, part=None):
    row, col = region(piece, ref, k, part)
    return ref.at[(L["l"], p, q, row, col) if L["l"] == 0 else (L["l"], q, p, row, col)]


def step_kernel(side, piece, per_weight, *refs):
    n_w = 3
    grads, weights, ms, vs = (refs[i * n_w : (i + 1) * n_w] for i in range(4))
    wholes, new_ms, new_vs = (refs[i * n_w : (i + 1) * n_w] for i in range(4, 7))
    onward = refs[7 * n_w : 7 * n_w + 4]
    (l1, l2, m1, m2, o1, o2, w_in, m_io, v_io, kept, kept_half, w_new,
     send_sem, r_sem, ag_sem, o1_sem, o2_sem, in_sem, out_sem, own_sem) = refs[7 * n_w + 4 :]
    rows, cols = piece
    half = cols // 2
    chunks = n_w * per_weight
    body = chunks - TAIL
    me = lax.axis_index("dp")
    x, y = me // side, me % side

    def at(px, py):
        return {"dp": px * side + py}

    xs = [(x + 1) % side, (x + side - 1) % side]
    ys = [(y + 1) % side, (y + side - 1) % side]
    along_x, along_y = [at(i, y) for i in xs], [at(x, i) for i in ys]

    barrier = pltpu.get_barrier_semaphore()
    for device in along_x + along_y:
        pl.semaphore_signal(barrier, inc=1, device_id=device, device_id_type=MESH)
    pl.semaphore_wait(barrier, 4)

    layers = [
        dict(l=0, p=x, q=y, ps=xs, qs=ys, first=along_x, second=along_y),
        dict(l=1, p=y, q=x, ps=ys, qs=xs, first=along_y, second=along_x),
    ]

    block = functools.partial(block_of, piece)

    def mine(ref, L, k):
        return ref.at[(L["l"], *region(piece, ref, k))]

    def part_of(ref, part):
        return ref.at[..., pl.ds(part * half, half)]

    def for_weight(c, fn):
        for i in range(n_w):
            pl.when(c // per_weight == i)(functools.partial(fn, i, c % per_weight))

    def send(src, dst, s_sem, d_sem, device):
        pltpu.make_async_remote_copy(src, dst, s_sem, d_sem, device_id=device, device_id_type=MESH).start()

    def wait(ref, sem):
        pltpu.make_async_copy(ref, ref, sem).wait()

    every = pl.ds(0, side)

    def stage1(L, c):
        l = L["l"]

        def go(i, k):
            far = (L["p"] + 2) % side
            for d in range(2):
                send(block(grads[i], L, far, every, k, 1 - d), l1.at[c, l, d], send_sem.at[c, l, 0], r_sem.at[c, l, 0], L["first"][d])
            for d in range(2):
                send(block(grads[i], L, L["ps"][d], every, k, d), part_of(l2.at[c, l, d], d), send_sem.at[c, l, 0], r_sem.at[c, l, 1], L["first"][d])
                pltpu.make_async_copy(block(grads[i], L, L["ps"][d], every, k, 1 - d), o1.at[c % 2, l, d], o1_sem.at[c % 2, l, d]).start()

        for_weight(c, go)

    def stage2(L, c):
        l = L["l"]
        for_weight(c, lambda i, k: pltpu.make_async_copy(block(grads[i], L, L["p"], every, k), o2.at[c % 2, l], o2_sem.at[c % 2, l]).start())
        wait(l1.at[c, l], r_sem.at[c, l, 0])
        for d in range(2):
            wait(o1.at[c % 2, l, d], o1_sem.at[c % 2, l, d])

            @pl.loop(0, side * (rows // 16))
            def _(j):
                b, r = j // (rows // 16), pl.ds(pl.multiple_of(j % (rows // 16) * 16, 16), 16)
                l1[c, l, d, b, r, :] = (l1[c, l, d, b, r, :].astype(F32) + o1[c % 2, l, d, b, r, :].astype(F32)).astype(BF16)

            send(l1.at[c, l, d], part_of(l2.at[c, l, d], 1 - d), send_sem.at[c, l, 0], r_sem.at[c, l, 1], L["first"][d])

    def stage3(L, c):
        l, q = L["l"], L["q"]
        wait(l2.at[c, l], r_sem.at[c, l, 1])
        wait(o2.at[c % 2, l], o2_sem.at[c % 2, l])
        low, high = pl.ds(0, half), pl.ds(half, half)

        def total(b, r, col):
            return l2[c, l, 0, b, r, col].astype(F32) + l2[c, l, 1, b, r, col].astype(F32) + o2[c % 2, l, b, r, col].astype(F32)

        far = (q + 2) % side

        @pl.loop(0, rows // 16)
        def _(j):
            r = pl.ds(pl.multiple_of(j * 16, 16), 16)
            for col in (low, high):
                kept[c % 3, l, r, col] = total(q, r, col)
                l2[c, l, 0, far, r, col] = total(far, r, col).astype(BF16)
            for d, (direct, later) in enumerate(((low, high), (high, low))):
                near = L["qs"][d]
                kept_half[c % 3, l, d, r, :] = total(near, r, later)
                l2[c, l, 0, near, r, direct] = total(near, r, direct).astype(BF16)

        for d in range(2):
            send(part_of(l2.at[c, l, 0, far], 1 - d), m1.at[c, l, d], send_sem.at[c, l, 1], r_sem.at[c, l, 2], L["second"][d])
        for d in range(2):
            send(part_of(l2.at[c, l, 0, L["qs"][d]], d), part_of(m2.at[c, l, d], d), send_sem.at[c, l, 1], r_sem.at[c, l, 3], L["second"][d])

    def stage4(L, c):
        l = L["l"]

        def load(i, k):
            for ref, buffer, s in (
                (block(weights[i], L, L["p"], L["q"], k), w_in, 0),
                (mine(ms[i], L, k), m_io, 1),
                (mine(vs[i], L, k), v_io, 2),
            ):
                pltpu.make_async_copy(ref, buffer.at[c % 2, l], in_sem.at[c % 2, l, s]).start()

        @pl.when(c >= 2)
        def _():
            wait(m_io.at[c % 2, l], out_sem.at[c % 2, l, 0])
            wait(v_io.at[c % 2, l], out_sem.at[c % 2, l, 1])

        for_weight(c, load)
        wait(m1.at[c, l], r_sem.at[c, l, 2])
        for d in range(2):

            @pl.loop(0, rows // 16)
            def _(j):
                r = pl.ds(pl.multiple_of(j * 16, 16), 16)
                m1[c, l, d, r, :] = (m1[c, l, d, r, :].astype(F32) + kept_half[c % 3, l, d, r, :]).astype(BF16)

            send(m1.at[c, l, d], part_of(m2.at[c, l, d], 1 - d), send_sem.at[c, l, 1], r_sem.at[c, l, 3], L["second"][d])

    def stage5(L, c):
        l = L["l"]
        wait(m2.at[c, l], r_sem.at[c, l, 3])
        for s, buffer in enumerate((w_in, m_io, v_io)):
            wait(buffer.at[c % 2, l], in_sem.at[c % 2, l, s])

        @pl.loop(0, rows // 16)
        def _(j):
            r = pl.ds(pl.multiple_of(j * 16, 16), 16)
            g = kept[c % 3, l, r, :] + m2[c, l, 0, r, :].astype(F32) + m2[c, l, 1, r, :].astype(F32)
            g = g.astype(BF16).astype(F32)
            w_new[c, l, r, :], m_io[c % 2, l, r, :], v_io[c % 2, l, r, :] = adamw(
                w_in[c % 2, l, r, :].astype(F32), m_io[c % 2, l, r, :], v_io[c % 2, l, r, :], g
            )

        def go(i, k):
            there = block(wholes[i], L, L["p"], L["q"], k)
            for d in range(2):
                send(w_new.at[c, l], there, send_sem.at[c, l, 2], ag_sem.at[c, l, d], L["second"][d])
            pltpu.make_async_copy(w_new.at[c, l], there, own_sem.at[c % 3, l]).start()
            pltpu.make_async_copy(m_io.at[c % 2, l], mine(new_ms[i], L, k), out_sem.at[c % 2, l, 0]).start()
            pltpu.make_async_copy(v_io.at[c % 2, l], mine(new_vs[i], L, k), out_sem.at[c % 2, l, 1]).start()

        for_weight(c, go)

    def stage6(L, c):
        l = L["l"]

        def go(i, k):
            for d in range(2):
                wait(w_new.at[c, l], ag_sem.at[c, l, d])
                there = block(wholes[i], L, L["p"], L["qs"][1 - d], k, 1 - d)
                send(there, there, send_sem.at[c, l, 2], ag_sem.at[c, l, 2 + d], L["second"][d])

        for_weight(c, go)

    def stage7(L, c):
        l = L["l"]
        wait(w_new.at[c, l], own_sem.at[c % 3, l])
        for d in range(2):
            wait(part_of(w_new.at[c, l], d), ag_sem.at[c, l, 2 + d])

        def go(i, k):
            @pl.when(c < body)
            def _():
                there = block(wholes[i], L, L["p"], every, k)
                for d in range(2):
                    send(there, there, send_sem.at[c, l, 3], ag_sem.at[c, l, 4 + d], L["first"][d])

            @pl.when(c >= body)
            def _():
                for d in range(2):
                    here, on = (block(wholes[i], L, L["p"], every, k, part) for part in (d, 1 - d))
                    send(on, onward[2 * l + d].at[jnp.maximum(c - body, 0)], send_sem.at[c, l, 3], ag_sem.at[c, l, 4 + d], L["first"][d])
                    send(here, here, send_sem.at[c, l, 3], ag_sem.at[c, l, 4 + d], L["first"][d])

        for_weight(c, go)

    def stage8(L, c):
        l = L["l"]

        for d in range(2):
            wait(o2.at[0, 0], ag_sem.at[c, l, 4 + d])

        def go(i, k):
            for d in range(2):
                there = block(wholes[i], L, L["ps"][1 - d], every, k, 1 - d)
                send(there, there, send_sem.at[c, l, 3], ag_sem.at[c, l, 6 + d], L["first"][d])

        pl.when(c < body)(lambda: for_weight(c, go))

    def stage9(L, c):
        l = L["l"]

        @pl.when(c < body)
        def _():
            for d in range(2):
                wait(o1.at[0, 0, 0], ag_sem.at[c, l, 6 + d])

    stages = (stage1, stage2, stage3, stage4, stage5, stage6, stage7, stage8, stage9)

    @pl.loop(0, chunks + STAGES - 1)
    def _(t):
        for s, stage in enumerate(stages):
            c = t - s

            @pl.when((c >= 0) & (c < chunks))
            def _():
                for L in layers:
                    stage(L, c)

    for L in layers:
        for c in (chunks - 2, chunks - 1):
            wait(m_io.at[c % 2, L["l"]], out_sem.at[c % 2, L["l"], 0])
            wait(v_io.at[c % 2, L["l"]], out_sem.at[c % 2, L["l"], 1])

    three, row, col = pl.ds(0, 3), pl.ds(0, rows), pl.ds(0, cols)

    @pl.loop(0, chunks)
    def _(c):
        for l in range(2):
            wait(wholes[0].at[l, three, every, row, col], send_sem.at[c, l, 0])
            wait(wholes[0].at[l, 0, three, row, col], send_sem.at[c, l, 1])
            wait(wholes[0].at[l, 0, three, row, col], send_sem.at[c, l, 2])
            pl.when(c < body)(lambda: wait(wholes[0].at[l, three, every, row, col], send_sem.at[c, l, 3]))
            pl.when(c >= body)(lambda: wait(wholes[0].at[l, pl.ds(0, 2), every, row, col], send_sem.at[c, l, 3]))


def stream(copies, buffer, in_sem, out_sem, ahead):
    slots = buffer.shape[0]

    def slot_of(i):
        return buffer.at[(i % slots, *(pl.ds(0, n) for n in copies[i][0].shape))]

    loads = [pltpu.make_async_copy(src, slot_of(i), in_sem.at[i % slots]) for i, (src, _) in enumerate(copies)]
    stores = [pltpu.make_async_copy(slot_of(i), dst, out_sem.at[i % slots]) for i, (_, dst) in enumerate(copies)]
    for i in range(len(copies) + ahead):
        if i < len(copies):
            if i >= slots:
                stores[i - slots].wait()
            loads[i].start()
        if i >= ahead:
            loads[i - ahead].wait()
            stores[i - ahead].start()
        yield (i + 1) / (len(copies) + ahead)
    for one in stores[-slots:]:
        one.wait()
    yield 2.0


def together(*streams):
    done = [0.0] * len(streams)
    while min(done) < 2.0:
        i = done.index(min(done))
        done[i] = next(streams[i])


def places(side):
    me = lax.axis_index("dp")
    x, y = me // side, me % side
    return [dict(l=0, p=x), dict(l=1, p=y)]


def deliver_kernel(side, piece, per_weight, *refs):
    n_w = 3
    wholes, onward, moments = refs[:n_w], refs[n_w : n_w + 4], refs[n_w + 4 : 3 * n_w + 4]
    outs, new_moments = refs[3 * n_w + 4 : 4 * n_w + 4], refs[4 * n_w + 4 : 6 * n_w + 4]
    buffer, moment_buffer, in_sem, out_sem, m_in_sem, m_out_sem = refs[6 * n_w + 4 :]
    chunks = n_w * per_weight
    body = chunks - TAIL
    every = pl.ds(0, side)
    copies = []
    for c in range(chunks):
        i, k = divmod(c, per_weight)
        for L in places(side):
            for away in range(side):
                p = (L["p"] + away) % side
                parts = [block_of(piece, ref, L, p, every, k) for ref in (wholes[i], outs[i])]
                if c < body or away == 0:
                    copies.append(parts)
                elif away != 2:
                    d = 0 if away == side - 1 else 1
                    copies.append([block_of(piece, ref, L, p, every, k, d) for ref in (wholes[i], outs[i])])
                    copies.append([onward[2 * L["l"] + d].at[c - body], block_of(piece, outs[i], L, p, every, k, 1 - d)])
    more = []
    for old, new in zip(moments, new_moments):
        for l in range(old.shape[0]):
            for k in range(per_weight):
                more.append([ref.at[(l, *region(piece, ref, k))] for ref in (old, new)])
    together(
        stream(copies, buffer, in_sem, out_sem, buffer.shape[0] // 2),
        stream(more, moment_buffer, m_in_sem, m_out_sem, moment_buffer.shape[0] // 2),
    )


def finish_kernel(side, piece, per_weight, *refs):
    n_w = 3
    brought, outs, sem = refs[n_w : n_w + 4], refs[n_w + 4 : 2 * n_w + 4], refs[2 * n_w + 4]
    body = n_w * per_weight - TAIL
    copies = []
    for c in range(body, n_w * per_weight):
        i, k = divmod(c, per_weight)
        for L in places(side):
            for d in range(2):
                there = block_of(piece, outs[i], L, (L["p"] + 2) % side, pl.ds(0, side), k, 1 - d)
                copies.append(pltpu.make_async_copy(brought[2 * L["l"] + d].at[c - body], there, sem.at[len(copies)]))
    for one in copies:
        one.start()
    for one in copies:
        one.wait()


def solution(mesh):
    n = mesh.shape["dp"]
    side = math.isqrt(n)

    def step(*arrays):
        terms, weights, m, v = (arrays[i : i + 3] for i in (0, 3, 6, 9))
        layers = m[0].shape[0]
        piece = tuple(min(one.shape[i] for one in m) for i in (1, 2))
        rows, cols = piece
        sizes = {one.shape[1] * one.shape[2] for one in m}
        assert side * side == n and side == 4 and layers == 2 and len(sizes) == 1
        per_weight = sizes.pop() // (rows * cols)
        chunks = 3 * per_weight

        def blocks(a, one):
            return a.reshape(layers, side, side, *one.shape[1:])

        inputs = [blocks(a, one) for a, one in zip(terms, m)] + [blocks(a, one) for a, one in zip(weights, m)] + [*m, *v]
        outs = [jax.ShapeDtypeStruct((layers, side, side, *one.shape[1:]), BF16) for one in m]
        moments = [jax.ShapeDtypeStruct(one.shape, F32) for one in (*m, *v)]
        half = cols // 2
        onward = [jax.ShapeDtypeStruct((TAIL, side, rows, half), BF16)] * 4
        dma = pltpu.SemaphoreType.DMA
        any_space = pl.BlockSpec(memory_space=pl.ANY)
        results = pl.pallas_call(
            functools.partial(step_kernel, side, piece, per_weight),
            out_shape=outs + moments + onward,
            in_specs=[any_space] * 12,
            out_specs=[any_space] * 13,
            scratch_shapes=[
                pltpu.VMEM((chunks, layers, 2, side, rows, half), BF16),
                pltpu.VMEM((chunks, layers, 2, side, rows, cols), BF16),
                pltpu.VMEM((chunks, layers, 2, rows, half), BF16),
                pltpu.VMEM((chunks, layers, 2, rows, cols), BF16),
                pltpu.VMEM((2, layers, 2, side, rows, half), BF16),
                pltpu.VMEM((2, layers, side, rows, cols), BF16),
                pltpu.VMEM((2, layers, rows, cols), BF16),
                pltpu.VMEM((2, layers, rows, cols), F32),
                pltpu.VMEM((2, layers, rows, cols), F32),
                pltpu.VMEM((3, layers, rows, cols), F32),
                pltpu.VMEM((3, layers, 2, rows, half), F32),
                pltpu.VMEM((chunks, layers, rows, cols), BF16),
                dma((chunks, layers, 4)),
                dma((chunks, layers, 4)),
                dma((chunks, layers, 8)),
                dma((2, layers, 2)),
                dma((2, layers)),
                dma((2, layers, 3)),
                dma((2, layers, 2)),
                dma((3, layers)),
            ],
            compiler_params=pltpu.CompilerParams(collective_id=0, has_side_effects=True, vmem_limit_bytes=63 * 2**20),
            name="step",
        )(*inputs)
        wholes, moments, onward = results[:3], results[3:9], results[9:]
        hops = [
            [(x * side + y, ((x + dx) % side) * side + (y + dy) % side) for x in range(side) for y in range(side)]
            for dx, dy in ((1, 0), (-1, 0), (0, 1), (0, -1))
        ]
        brought = [lax.ppermute(one, "dp", hop) for one, hop in zip(onward, hops)]
        delivered = pl.pallas_call(
            functools.partial(deliver_kernel, side, piece, per_weight),
            out_shape=outs + [jax.ShapeDtypeStruct(one.shape, F32) for one in moments],
            in_specs=[any_space] * 13,
            out_specs=[any_space] * 9,
            scratch_shapes=[
                pltpu.VMEM((32, side, rows, cols), BF16),
                pltpu.VMEM((32, rows, cols), F32),
                dma((32,)),
                dma((32,)),
                dma((32,)),
                dma((32,)),
            ],
            compiler_params=pltpu.CompilerParams(vmem_limit_bytes=57 * 2**20),
            cost_estimate=pl.CostEstimate(flops=10**9, bytes_accessed=10**8, transcendentals=0),
            name="deliver",
        )(*wholes, *onward, *moments)
        whole = pl.pallas_call(
            functools.partial(finish_kernel, side, piece, per_weight),
            out_shape=outs,
            in_specs=[any_space] * 3 + [pl.BlockSpec(memory_space=pltpu.VMEM)] * 4,
            out_specs=[any_space] * 3,
            input_output_aliases={0: 0, 1: 1, 2: 2},
            scratch_shapes=[dma((4 * TAIL,))],
            compiler_params=pltpu.CompilerParams(vmem_limit_bytes=16 * 2**20),
            name="finish",
        )(*delivered[:3], *brought)
        whole = [r.reshape(a.shape) for r, a in zip(whole, weights)]
        return (*whole, *delivered[3:])

    all_of, cut = P(None, None, None), P(None, "dp", None)
    return jax.shard_map(
        step,
        mesh=mesh,
        in_specs=(P(("rep", "dp"), None, None, None),) * 3 + (all_of,) * 3 + (cut,) * 6,
        out_specs=(P("rep", None, None),) * 3 + (P("rep", "dp", None),) * 6,
        check_vma=False,
    )
```

```python
import functools
import math

import jax
import jax.numpy as jnp
from jax import lax
from jax.experimental import pallas as pl
from jax.experimental.pallas import tpu as pltpu
from jax.sharding import PartitionSpec as P

MESH = pl.DeviceIdType.MESH
F32, BF16 = jnp.float32, jnp.bfloat16
STAGES = 9
TAILS = (8, 2)
TAIL = sum(TAILS)
VMEM = 67043328


def adamw(w, m, v, g):
    m = 0.9 * m + 0.1 * g
    v = 0.95 * v + 0.05 * g * g
    step = m * lax.rsqrt(v + 1e-8) + 0.1 * w
    return (w - 0.02 * step).astype(BF16), m, v


def aligned(start, size):
    return pl.ds(start if isinstance(start, int) else pl.multiple_of(start, size), size)


def region(piece, ref, k, part=None):
    rows, cols = piece
    across = ref.shape[-1] // cols
    row, col = k // across * rows, k % across * cols
    if part is None:
        return aligned(row, rows), aligned(col, cols)
    return aligned(row, rows), aligned(col + part * (cols // 2), cols // 2)


def block_of(piece, ref, L, p, q, k, part=None):
    row, col = region(piece, ref, k, part)
    return ref.at[(L["l"], p, q, row, col) if L["l"] == 0 else (L["l"], q, p, row, col)]


def step_kernel(side, piece, per_weight, *refs):
    n_w = 3
    grads, weights, ms, vs = (refs[i * n_w : (i + 1) * n_w] for i in range(4))
    wholes, new_ms, new_vs = (refs[i * n_w : (i + 1) * n_w] for i in range(4, 7))
    n_on = 4 * len(TAILS)
    onward = refs[7 * n_w : 7 * n_w + n_on]
    (l1, l2, m1, m2, o1, o2, w_in, m_io, v_io, kept, kept_half, w_new,
     send_sem, r_sem, ag_sem, o1_sem, o2_sem, in_sem, out_sem, own_sem) = refs[7 * n_w + n_on :]
    rows, cols = piece
    half = cols // 2
    chunks = n_w * per_weight
    body = chunks - TAIL
    me = lax.axis_index("dp")
    x, y = me // side, me % side

    def at(px, py):
        return {"dp": px * side + py}

    xs = [(x + 1) % side, (x + side - 1) % side]
    ys = [(y + 1) % side, (y + side - 1) % side]
    along_x, along_y = [at(i, y) for i in xs], [at(x, i) for i in ys]

    barrier = pltpu.get_barrier_semaphore()
    for device in along_x + along_y:
        pl.semaphore_signal(barrier, inc=1, device_id=device, device_id_type=MESH)
    pl.semaphore_wait(barrier, 4)

    pl.when(lax.axis_index("rep") % 2 == 1)(lambda: pl.delay(10000))
    layers = [
        dict(l=0, p=x, q=y, ps=xs, qs=ys, first=along_x, second=along_y),
        dict(l=1, p=y, q=x, ps=ys, qs=xs, first=along_y, second=along_x),
    ]

    block = functools.partial(block_of, piece)

    def mine(ref, L, k):
        return ref.at[(L["l"], *region(piece, ref, k))]

    def part_of(ref, part):
        return ref.at[..., pl.ds(part * half, half)]

    def for_weight(c, fn):
        for i in range(n_w):
            pl.when(c // per_weight == i)(functools.partial(fn, i, c % per_weight))

    def send(src, dst, s_sem, d_sem, device):
        pltpu.make_async_remote_copy(src, dst, s_sem, d_sem, device_id=device, device_id_type=MESH).start()

    def wait(ref, sem):
        pltpu.make_async_copy(ref, ref, sem).wait()

    every = pl.ds(0, side)

    def stage1(L, c):
        l = L["l"]

        def go(i, k):
            far = (L["p"] + 2) % side
            for d in range(2):
                send(block(grads[i], L, far, every, k, 1 - d), l1.at[c, l, d], send_sem.at[c, l, 0], r_sem.at[c, l, 0], L["first"][d])
            for d in range(2):
                send(block(grads[i], L, L["ps"][d], every, k, d), part_of(l2.at[c, l, d], d), send_sem.at[c, l, 0], r_sem.at[c, l, 1], L["first"][d])
                pltpu.make_async_copy(block(grads[i], L, L["ps"][d], every, k, 1 - d), o1.at[c % 2, l, d], o1_sem.at[c % 2, l, d]).start()

        for_weight(c, go)

    def stage2(L, c):
        l = L["l"]
        for_weight(c, lambda i, k: pltpu.make_async_copy(block(grads[i], L, L["p"], every, k), o2.at[c % 2, l], o2_sem.at[c % 2, l]).start())
        wait(l1.at[c, l], r_sem.at[c, l, 0])
        for d in range(2):
            wait(o1.at[c % 2, l, d], o1_sem.at[c % 2, l, d])

            @pl.loop(0, side * (rows // 16))
            def _(j):
                b, r = j // (rows // 16), pl.ds(pl.multiple_of(j % (rows // 16) * 16, 16), 16)
                l1[c, l, d, b, r, :] = (l1[c, l, d, b, r, :].astype(F32) + o1[c % 2, l, d, b, r, :].astype(F32)).astype(BF16)

            send(l1.at[c, l, d], part_of(l2.at[c, l, d], 1 - d), send_sem.at[c, l, 0], r_sem.at[c, l, 1], L["first"][d])

    def stage3(L, c):
        l, q = L["l"], L["q"]
        wait(l2.at[c, l], r_sem.at[c, l, 1])
        wait(o2.at[c % 2, l], o2_sem.at[c % 2, l])
        low, high = pl.ds(0, half), pl.ds(half, half)

        def total(b, r, col):
            return l2[c, l, 0, b, r, col].astype(F32) + l2[c, l, 1, b, r, col].astype(F32) + o2[c % 2, l, b, r, col].astype(F32)

        far = (q + 2) % side

        @pl.loop(0, rows // 16)
        def _(j):
            r = pl.ds(pl.multiple_of(j * 16, 16), 16)
            for col in (low, high):
                kept[c % 3, l, r, col] = total(q, r, col)
                l2[c, l, 0, far, r, col] = total(far, r, col).astype(BF16)
            for d, (direct, later) in enumerate(((low, high), (high, low))):
                near = L["qs"][d]
                kept_half[c % 3, l, d, r, :] = total(near, r, later)
                l2[c, l, 0, near, r, direct] = total(near, r, direct).astype(BF16)

        for d in range(2):
            send(part_of(l2.at[c, l, 0, far], 1 - d), m1.at[c, l, d], send_sem.at[c, l, 1], r_sem.at[c, l, 2], L["second"][d])
        for d in range(2):
            send(part_of(l2.at[c, l, 0, L["qs"][d]], d), part_of(m2.at[c, l, d], d), send_sem.at[c, l, 1], r_sem.at[c, l, 3], L["second"][d])

    def stage4(L, c):
        l = L["l"]

        def load(i, k):
            for ref, buffer, s in (
                (block(weights[i], L, L["p"], L["q"], k), w_in, 0),
                (mine(ms[i], L, k), m_io, 1),
                (mine(vs[i], L, k), v_io, 2),
            ):
                pltpu.make_async_copy(ref, buffer.at[c % 2, l], in_sem.at[c % 2, l, s]).start()

        @pl.when(c >= 2)
        def _():
            wait(m_io.at[c % 2, l], out_sem.at[c % 2, l, 0])
            wait(v_io.at[c % 2, l], out_sem.at[c % 2, l, 1])

        for_weight(c, load)
        wait(m1.at[c, l], r_sem.at[c, l, 2])
        for d in range(2):

            @pl.loop(0, rows // 16)
            def _(j):
                r = pl.ds(pl.multiple_of(j * 16, 16), 16)
                m1[c, l, d, r, :] = (m1[c, l, d, r, :].astype(F32) + kept_half[c % 3, l, d, r, :]).astype(BF16)

            send(m1.at[c, l, d], part_of(m2.at[c, l, d], 1 - d), send_sem.at[c, l, 1], r_sem.at[c, l, 3], L["second"][d])

    def stage5(L, c):
        l = L["l"]
        wait(m2.at[c, l], r_sem.at[c, l, 3])
        for s, buffer in enumerate((w_in, m_io, v_io)):
            wait(buffer.at[c % 2, l], in_sem.at[c % 2, l, s])

        @pl.loop(0, rows // 16)
        def _(j):
            r = pl.ds(pl.multiple_of(j * 16, 16), 16)
            g = kept[c % 3, l, r, :] + m2[c, l, 0, r, :].astype(F32) + m2[c, l, 1, r, :].astype(F32)
            g = g.astype(BF16).astype(F32)
            w_new[c, l, r, :], m_io[c % 2, l, r, :], v_io[c % 2, l, r, :] = adamw(
                w_in[c % 2, l, r, :].astype(F32), m_io[c % 2, l, r, :], v_io[c % 2, l, r, :], g
            )

        def go(i, k):
            there = block(wholes[i], L, L["p"], L["q"], k)
            for d in range(2):
                send(w_new.at[c, l], there, send_sem.at[c, l, 2], ag_sem.at[c, l, d], L["second"][d])
            pltpu.make_async_copy(w_new.at[c, l], there, own_sem.at[c % 3, l]).start()
            pltpu.make_async_copy(m_io.at[c % 2, l], mine(new_ms[i], L, k), out_sem.at[c % 2, l, 0]).start()
            pltpu.make_async_copy(v_io.at[c % 2, l], mine(new_vs[i], L, k), out_sem.at[c % 2, l, 1]).start()

        for_weight(c, go)

    def stage6(L, c):
        l = L["l"]

        def go(i, k):
            for d in range(2):
                wait(w_new.at[c, l], ag_sem.at[c, l, d])
                there = block(wholes[i], L, L["p"], L["qs"][1 - d], k, 1 - d)
                send(there, there, send_sem.at[c, l, 2], ag_sem.at[c, l, 2 + d], L["second"][d])

        for_weight(c, go)

    def stage7(L, c):
        l = L["l"]
        wait(w_new.at[c, l], own_sem.at[c % 3, l])
        for d in range(2):
            wait(part_of(w_new.at[c, l], d), ag_sem.at[c, l, 2 + d])

        def go(i, k):
            @pl.when(c < body)
            def _():
                there = block(wholes[i], L, L["p"], every, k)
                for d in range(2):
                    send(there, there, send_sem.at[c, l, 3], ag_sem.at[c, l, 4 + d], L["first"][d])

            def end(j, start, size):
                for d in range(2):
                    here, on = (block(wholes[i], L, L["p"], every, k, part) for part in (d, 1 - d))
                    there = onward[4 * j + 2 * l + d].at[jnp.clip(c - start, 0, size - 1)]
                    send(on, there, send_sem.at[c, l, 3], ag_sem.at[c, l, 4 + d], L["first"][d])
                    send(here, here, send_sem.at[c, l, 3], ag_sem.at[c, l, 4 + d], L["first"][d])

            for j, size in enumerate(TAILS):
                start = body + sum(TAILS[:j])
                pl.when((c >= start) & (c < start + size))(functools.partial(end, j, start, size))

        for_weight(c, go)

    def stage8(L, c):
        l = L["l"]

        for d in range(2):
            wait(o2.at[0, 0], ag_sem.at[c, l, 4 + d])

        def go(i, k):
            for d in range(2):
                there = block(wholes[i], L, L["ps"][1 - d], every, k, 1 - d)
                send(there, there, send_sem.at[c, l, 3], ag_sem.at[c, l, 6 + d], L["first"][d])

        pl.when(c < body)(lambda: for_weight(c, go))

    def stage9(L, c):
        l = L["l"]

        @pl.when(c < body)
        def _():
            for d in range(2):
                wait(o1.at[0, 0, 0], ag_sem.at[c, l, 6 + d])

    stages = (stage1, stage2, stage3, stage4, stage5, stage6, stage7, stage8, stage9)

    @pl.loop(0, chunks + STAGES - 1)
    def _(t):
        for s, stage in enumerate(stages):
            c = t - s

            @pl.when((c >= 0) & (c < chunks))
            def _():
                for L in layers:
                    stage(L, c)

    for L in layers:
        for c in (chunks - 2, chunks - 1):
            wait(m_io.at[c % 2, L["l"]], out_sem.at[c % 2, L["l"], 0])
            wait(v_io.at[c % 2, L["l"]], out_sem.at[c % 2, L["l"], 1])

    three, row, col = pl.ds(0, 3), pl.ds(0, rows), pl.ds(0, cols)

    @pl.loop(0, chunks)
    def _(c):
        for l in range(2):
            wait(wholes[0].at[l, three, every, row, col], send_sem.at[c, l, 0])
            wait(wholes[0].at[l, 0, three, row, col], send_sem.at[c, l, 1])
            wait(wholes[0].at[l, 0, three, row, col], send_sem.at[c, l, 2])
            pl.when(c < body)(lambda: wait(wholes[0].at[l, three, every, row, col], send_sem.at[c, l, 3]))
            pl.when(c >= body)(lambda: wait(wholes[0].at[l, pl.ds(0, 2), every, row, col], send_sem.at[c, l, 3]))


def stream(copies, buffer, in_sem, out_sem, ahead):
    slots = buffer.shape[0]

    def slot_of(i):
        return buffer.at[(i % slots, *(pl.ds(0, n) for n in copies[i][0].shape))]

    loads = [pltpu.make_async_copy(src, slot_of(i), in_sem.at[i % slots]) for i, (src, _) in enumerate(copies)]
    stores = [pltpu.make_async_copy(slot_of(i), dst, out_sem.at[i % slots]) for i, (_, dst) in enumerate(copies)]
    for i in range(len(copies) + ahead):
        if i < len(copies):
            if i >= slots:
                stores[i - slots].wait()
            loads[i].start()
        if i >= ahead:
            loads[i - ahead].wait()
            stores[i - ahead].start()
        yield (i + 1) / (len(copies) + ahead)
    for one in stores[-slots:]:
        one.wait()
    yield 2.0


def together(*streams):
    done = [0.0] * len(streams)
    while min(done) < 2.0:
        i = done.index(min(done))
        done[i] = next(streams[i])


def places(side):
    me = lax.axis_index("dp")
    x, y = me // side, me % side
    return [dict(l=0, p=x), dict(l=1, p=y)]


def place_in_tail(at):
    j = 0
    while at >= TAILS[j]:
        at -= TAILS[j]
        j += 1
    return j, at


def deliver_kernel(side, piece, per_weight, *refs):
    n_w = 3
    n_on = 4 * len(TAILS)
    wholes, onward, moments = refs[:n_w], refs[n_w : n_w + n_on], refs[n_w + n_on : 3 * n_w + n_on]
    refs = refs[3 * n_w + n_on :]
    outs, new_moments = refs[:n_w], refs[n_w : 3 * n_w]
    buffer, moment_buffer, in_sem, out_sem, m_in_sem, m_out_sem = refs[3 * n_w + n_on - 4 :]
    chunks = n_w * per_weight
    body = chunks - TAIL
    every = pl.ds(0, side)
    copies = []
    for c in range(chunks):
        i, k = divmod(c, per_weight)
        for L in places(side):
            for away in range(side):
                p = (L["p"] + away) % side
                parts = [block_of(piece, ref, L, p, every, k) for ref in (wholes[i], outs[i])]
                if c < body or away == 0:
                    copies.append(parts)
                elif away != 2:
                    d = 0 if away == side - 1 else 1
                    copies.append([block_of(piece, ref, L, p, every, k, d) for ref in (wholes[i], outs[i])])
                    j, at = place_in_tail(c - body)
                    copies.append([onward[4 * j + 2 * L["l"] + d].at[at], block_of(piece, outs[i], L, p, every, k, 1 - d)])
    more = []
    for old, new in zip(moments, new_moments):
        for l in range(old.shape[0]):
            for k in range(per_weight):
                more.append([ref.at[(l, *region(piece, ref, k))] for ref in (old, new)])
    together(
        stream(copies, buffer, in_sem, out_sem, buffer.shape[0] // 2),
        stream(more, moment_buffer, m_in_sem, m_out_sem, moment_buffer.shape[0] // 2),
    )


def finish_kernel(side, piece, per_weight, which, *refs):
    n_w = 3
    brought, outs, sem = refs[n_w : n_w + 4], refs[n_w + 4 : 2 * n_w + 4], refs[2 * n_w + 4]
    copies = []
    for c in range(n_w * per_weight - TAIL, n_w * per_weight):
        i, k = divmod(c, per_weight)
        j, at = place_in_tail(c - n_w * per_weight + TAIL)
        if j == which:
            for L in places(side):
                for d in range(2):
                    there = block_of(piece, outs[i], L, (L["p"] + 2) % side, pl.ds(0, side), k, 1 - d)
                    copies.append(pltpu.make_async_copy(brought[2 * L["l"] + d].at[at], there, sem.at[len(copies)]))
    for one in copies:
        one.start()
    for one in copies:
        one.wait()


def solution(mesh):
    n = mesh.shape["dp"]
    side = math.isqrt(n)

    def step(*arrays):
        terms, weights, m, v = (arrays[i : i + 3] for i in (0, 3, 6, 9))
        layers = m[0].shape[0]
        rows, cols = piece = min(one.shape[1] for one in m), min(one.shape[2] for one in m)
        sizes = {one.shape[1] * one.shape[2] for one in m}
        assert side * side == n and side == 4 and layers == 2 and len(sizes) == 1
        per_weight = sizes.pop() // (rows * cols)
        chunks = 3 * per_weight

        def blocks(a, one):
            return a.reshape(layers, side, side, *one.shape[1:])

        inputs = [blocks(a, one) for a, one in zip(terms, m)] + [blocks(a, one) for a, one in zip(weights, m)] + [*m, *v]
        outs = [jax.ShapeDtypeStruct((layers, side, side, *one.shape[1:]), BF16) for one in m]
        moments = [jax.ShapeDtypeStruct(one.shape, F32) for one in (*m, *v)]
        half = cols // 2
        onward = [jax.ShapeDtypeStruct((size, side, rows, half), BF16) for size in TAILS for _ in range(4)]
        dma = pltpu.SemaphoreType.DMA
        any_space = pl.BlockSpec(memory_space=pl.ANY)
        results = pl.pallas_call(
            functools.partial(step_kernel, side, piece, per_weight),
            out_shape=outs + moments + onward,
            in_specs=[any_space] * 12,
            out_specs=[any_space] * (9 + len(onward)),
            scratch_shapes=[
                pltpu.VMEM((chunks, layers, 2, side, rows, half), BF16),
                pltpu.VMEM((chunks, layers, 2, side, rows, cols), BF16),
                pltpu.VMEM((chunks, layers, 2, rows, half), BF16),
                pltpu.VMEM((chunks, layers, 2, rows, cols), BF16),
                pltpu.VMEM((2, layers, 2, side, rows, half), BF16),
                pltpu.VMEM((2, layers, side, rows, cols), BF16),
                pltpu.VMEM((2, layers, rows, cols), BF16),
                pltpu.VMEM((2, layers, rows, cols), F32),
                pltpu.VMEM((2, layers, rows, cols), F32),
                pltpu.VMEM((3, layers, rows, cols), F32),
                pltpu.VMEM((3, layers, 2, rows, half), F32),
                pltpu.VMEM((chunks, layers, rows, cols), BF16),
                dma((chunks, layers, 4)),
                dma((chunks, layers, 4)),
                dma((chunks, layers, 8)),
                dma((2, layers, 2)),
                dma((2, layers)),
                dma((2, layers, 3)),
                dma((2, layers, 2)),
                dma((3, layers)),
            ],
            compiler_params=pltpu.CompilerParams(collective_id=0, has_side_effects=True, vmem_limit_bytes=63 * 2**20),
            name="step",
        )(*inputs)
        wholes, moments, onward = results[:3], results[3:9], results[9:]
        hops = [
            [(x * side + y, ((x + dx) % side) * side + (y + dy) % side) for x in range(side) for y in range(side)]
            for dx, dy in ((1, 0), (-1, 0), (0, 1), (0, -1))
        ]
        brought = [lax.ppermute(one, "dp", hop) for one, hop in zip(onward[:4], hops)]
        delivered = pl.pallas_call(
            functools.partial(deliver_kernel, side, piece, per_weight),
            out_shape=outs + [jax.ShapeDtypeStruct(one.shape, one.dtype) for one in (*moments, *onward[4:])],
            in_specs=[any_space] * (9 + len(onward)),
            out_specs=[any_space] * (5 + len(onward)),
            input_output_aliases={7 + i: 9 + i for i in range(len(onward) - 4)},
            scratch_shapes=[
                pltpu.VMEM((32, side, rows, cols), BF16),
                pltpu.VMEM((32, rows, cols), F32),
                *[dma((32,))] * 4,
            ],
            compiler_params=pltpu.CompilerParams(vmem_limit_bytes=VMEM - 8 * TAILS[0] * side * rows * half - 2**17),
            cost_estimate=pl.CostEstimate(flops=10**9, bytes_accessed=10**8, transcendentals=0),
            name="deliver",
        )(*wholes, *onward, *moments)
        brought += [lax.ppermute(one, "dp", hop) for one, hop in zip(delivered[9:], hops * (len(TAILS) - 1))]
        whole = delivered[:3]
        for j, size in enumerate(TAILS):
            whole = pl.pallas_call(
                functools.partial(finish_kernel, side, piece, per_weight, j),
                out_shape=outs,
                in_specs=[any_space] * 3 + [pl.BlockSpec(memory_space=pltpu.VMEM)] * 4,
                out_specs=[any_space] * 3,
                input_output_aliases={0: 0, 1: 1, 2: 2},
                scratch_shapes=[dma((4 * size,))],
                compiler_params=pltpu.CompilerParams(vmem_limit_bytes=16 * 2**20),
                name="finish",
            )(*whole, *brought[4 * j : 4 * j + 4])
        whole = [r.reshape(a.shape) for r, a in zip(whole, weights)]
        return (*whole, *delivered[3:9])

    all_of, cut = P(None, None, None), P(None, "dp", None)
    return jax.shard_map(
        step,
        mesh=mesh,
        in_specs=(P(("rep", "dp"), None, None, None),) * 3 + (all_of,) * 3 + (cut,) * 6,
        out_specs=(P("rep", None, None),) * 3 + (P("rep", "dp", None),) * 6,
        check_vma=False,
    )
```

```python
import functools
import math

import jax
import jax.numpy as jnp
from jax import lax
from jax.experimental import pallas as pl
from jax.experimental.pallas import tpu as pltpu
from jax.sharding import PartitionSpec as P

MESH = pl.DeviceIdType.MESH
F32, BF16 = jnp.float32, jnp.bfloat16
STAGES = 9
TAILS = (8, 2)
TAIL = sum(TAILS)
VMEM = 67043328


def adamw(w, m, v, g):
    m = 0.9 * m + 0.1 * g
    v = 0.95 * v + 0.05 * g * g
    step = m * lax.rsqrt(v + 1e-8) + 0.1 * w
    return (w - 0.02 * step).astype(BF16), m, v


def aligned(start, size):
    return pl.ds(start if isinstance(start, int) else pl.multiple_of(start, size), size)


def region(piece, ref, k, part=None):
    rows, cols = piece
    across = ref.shape[-1] // cols
    row, col = k // across * rows, k % across * cols
    if part is None:
        return aligned(row, rows), aligned(col, cols)
    return aligned(row, rows), aligned(col + part * (cols // 2), cols // 2)


def block_of(piece, ref, L, p, q, k, part=None):
    row, col = region(piece, ref, k, part)
    return ref.at[(L["l"], p, q, row, col) if L["l"] == 0 else (L["l"], q, p, row, col)]


def step_kernel(side, piece, per_weight, *refs):
    n_w = 3
    grads, weights, ms, vs = (refs[i * n_w : (i + 1) * n_w] for i in range(4))
    wholes, new_ms, new_vs = (refs[i * n_w : (i + 1) * n_w] for i in range(4, 7))
    n_on = 4 * len(TAILS)
    onward = refs[7 * n_w : 7 * n_w + n_on]
    (l1, l2, m1, m2, o1, o2, w_in, m_io, v_io, kept, kept_half, w_new,
     send_sem, r_sem, ag_sem, o1_sem, o2_sem, in_sem, out_sem, own_sem) = refs[7 * n_w + n_on :]
    rows, cols = piece
    half = cols // 2
    chunks = n_w * per_weight
    body = chunks - TAIL
    me = lax.axis_index("dp")
    x, y = me // side, me % side

    def at(px, py):
        return {"dp": px * side + py}

    xs = [(x + 1) % side, (x + side - 1) % side]
    ys = [(y + 1) % side, (y + side - 1) % side]
    along_x, along_y = [at(i, y) for i in xs], [at(x, i) for i in ys]

    barrier = pltpu.get_barrier_semaphore()
    for device in along_x + along_y:
        pl.semaphore_signal(barrier, inc=1, device_id=device, device_id_type=MESH)
    pl.semaphore_wait(barrier, 4)

    pl.when(lax.axis_index("rep") % 2 == 1)(lambda: pl.delay(12000))
    layers = [
        dict(l=0, p=x, q=y, ps=xs, qs=ys, first=along_x, second=along_y),
        dict(l=1, p=y, q=x, ps=ys, qs=xs, first=along_y, second=along_x),
    ]

    block = functools.partial(block_of, piece)

    def mine(ref, L, k):
        return ref.at[(L["l"], *region(piece, ref, k))]

    def part_of(ref, part):
        return ref.at[..., pl.ds(part * half, half)]

    def for_weight(c, fn):
        for i in range(n_w):
            pl.when(c // per_weight == i)(functools.partial(fn, i, c % per_weight))

    def send(src, dst, s_sem, d_sem, device):
        pltpu.make_async_remote_copy(src, dst, s_sem, d_sem, device_id=device, device_id_type=MESH).start()

    def wait(ref, sem):
        pltpu.make_async_copy(ref, ref, sem).wait()

    every = pl.ds(0, side)

    def stage1(L, c):
        l = L["l"]

        def go(i, k):
            far = (L["p"] + 2) % side
            for d in range(2):
                send(block(grads[i], L, far, every, k, 1 - d), l1.at[c, l, d], send_sem.at[c, l, 0], r_sem.at[c, l, 0], L["first"][d])
            for d in range(2):
                send(block(grads[i], L, L["ps"][d], every, k, d), part_of(l2.at[c, l, d], d), send_sem.at[c, l, 0], r_sem.at[c, l, 1], L["first"][d])
                pltpu.make_async_copy(block(grads[i], L, L["ps"][d], every, k, 1 - d), o1.at[c % 2, l, d], o1_sem.at[c % 2, l, d]).start()

        for_weight(c, go)

    def stage2(L, c):
        l = L["l"]
        for_weight(c, lambda i, k: pltpu.make_async_copy(block(grads[i], L, L["p"], every, k), o2.at[c % 2, l], o2_sem.at[c % 2, l]).start())
        wait(l1.at[c, l], r_sem.at[c, l, 0])
        for d in range(2):
            wait(o1.at[c % 2, l, d], o1_sem.at[c % 2, l, d])

            @pl.loop(0, side * (rows // 16))
            def _(j):
                b, r = j // (rows // 16), pl.ds(pl.multiple_of(j % (rows // 16) * 16, 16), 16)
                l1[c, l, d, b, r, :] = (l1[c, l, d, b, r, :].astype(F32) + o1[c % 2, l, d, b, r, :].astype(F32)).astype(BF16)

            send(l1.at[c, l, d], part_of(l2.at[c, l, d], 1 - d), send_sem.at[c, l, 0], r_sem.at[c, l, 1], L["first"][d])

    def stage3(L, c):
        l, q = L["l"], L["q"]
        wait(l2.at[c, l], r_sem.at[c, l, 1])
        wait(o2.at[c % 2, l], o2_sem.at[c % 2, l])
        low, high = pl.ds(0, half), pl.ds(half, half)

        def total(b, r, col):
            return l2[c, l, 0, b, r, col].astype(F32) + l2[c, l, 1, b, r, col].astype(F32) + o2[c % 2, l, b, r, col].astype(F32)

        far = (q + 2) % side

        @pl.loop(0, rows // 16)
        def _(j):
            r = pl.ds(pl.multiple_of(j * 16, 16), 16)
            for col in (low, high):
                kept[c % 3, l, r, col] = total(q, r, col)
                l2[c, l, 0, far, r, col] = total(far, r, col).astype(BF16)
            for d, (direct, later) in enumerate(((low, high), (high, low))):
                near = L["qs"][d]
                kept_half[c % 3, l, d, r, :] = total(near, r, later)
                l2[c, l, 0, near, r, direct] = total(near, r, direct).astype(BF16)

        for d in range(2):
            send(part_of(l2.at[c, l, 0, far], 1 - d), m1.at[c, l, d], send_sem.at[c, l, 1], r_sem.at[c, l, 2], L["second"][d])
        for d in range(2):
            send(part_of(l2.at[c, l, 0, L["qs"][d]], d), part_of(m2.at[c, l, d], d), send_sem.at[c, l, 1], r_sem.at[c, l, 3], L["second"][d])

    def stage4(L, c):
        l = L["l"]

        def load(i, k):
            for ref, buffer, s in (
                (block(weights[i], L, L["p"], L["q"], k), w_in, 0),
                (mine(ms[i], L, k), m_io, 1),
                (mine(vs[i], L, k), v_io, 2),
            ):
                pltpu.make_async_copy(ref, buffer.at[c % 2, l], in_sem.at[c % 2, l, s]).start()

        @pl.when(c >= 2)
        def _():
            wait(m_io.at[c % 2, l], out_sem.at[c % 2, l, 0])
            wait(v_io.at[c % 2, l], out_sem.at[c % 2, l, 1])

        for_weight(c, load)
        wait(m1.at[c, l], r_sem.at[c, l, 2])
        for d in range(2):

            @pl.loop(0, rows // 16)
            def _(j):
                r = pl.ds(pl.multiple_of(j * 16, 16), 16)
                m1[c, l, d, r, :] = (m1[c, l, d, r, :].astype(F32) + kept_half[c % 3, l, d, r, :]).astype(BF16)

            send(m1.at[c, l, d], part_of(m2.at[c, l, d], 1 - d), send_sem.at[c, l, 1], r_sem.at[c, l, 3], L["second"][d])

    def stage5(L, c):
        l = L["l"]
        wait(m2.at[c, l], r_sem.at[c, l, 3])
        for s, buffer in enumerate((w_in, m_io, v_io)):
            wait(buffer.at[c % 2, l], in_sem.at[c % 2, l, s])

        @pl.loop(0, rows // 16)
        def _(j):
            r = pl.ds(pl.multiple_of(j * 16, 16), 16)
            g = kept[c % 3, l, r, :] + m2[c, l, 0, r, :].astype(F32) + m2[c, l, 1, r, :].astype(F32)
            g = g.astype(BF16).astype(F32)
            w_new[c, l, r, :], m_io[c % 2, l, r, :], v_io[c % 2, l, r, :] = adamw(
                w_in[c % 2, l, r, :].astype(F32), m_io[c % 2, l, r, :], v_io[c % 2, l, r, :], g
            )

        def go(i, k):
            there = block(wholes[i], L, L["p"], L["q"], k)
            for d in range(2):
                send(w_new.at[c, l], there, send_sem.at[c, l, 2], ag_sem.at[c, l, d], L["second"][d])
            pltpu.make_async_copy(w_new.at[c, l], there, own_sem.at[c % 3, l]).start()
            pltpu.make_async_copy(m_io.at[c % 2, l], mine(new_ms[i], L, k), out_sem.at[c % 2, l, 0]).start()
            pltpu.make_async_copy(v_io.at[c % 2, l], mine(new_vs[i], L, k), out_sem.at[c % 2, l, 1]).start()

        for_weight(c, go)

    def stage6(L, c):
        l = L["l"]

        def go(i, k):
            for d in range(2):
                wait(w_new.at[c, l], ag_sem.at[c, l, d])
                there = block(wholes[i], L, L["p"], L["qs"][1 - d], k, 1 - d)
                send(there, there, send_sem.at[c, l, 2], ag_sem.at[c, l, 2 + d], L["second"][d])

        for_weight(c, go)

    def stage7(L, c):
        l = L["l"]
        wait(w_new.at[c, l], own_sem.at[c % 3, l])
        for d in range(2):
            wait(part_of(w_new.at[c, l], d), ag_sem.at[c, l, 2 + d])

        def go(i, k):
            @pl.when(c < body)
            def _():
                there = block(wholes[i], L, L["p"], every, k)
                for d in range(2):
                    send(there, there, send_sem.at[c, l, 3], ag_sem.at[c, l, 4 + d], L["first"][d])

            def end(j, start, size):
                for d in range(2):
                    here, on = (block(wholes[i], L, L["p"], every, k, part) for part in (d, 1 - d))
                    there = onward[4 * j + 2 * l + d].at[jnp.clip(c - start, 0, size - 1)]
                    send(on, there, send_sem.at[c, l, 3], ag_sem.at[c, l, 4 + d], L["first"][d])
                    send(here, here, send_sem.at[c, l, 3], ag_sem.at[c, l, 4 + d], L["first"][d])

            for j, size in enumerate(TAILS):
                start = body + sum(TAILS[:j])
                pl.when((c >= start) & (c < start + size))(functools.partial(end, j, start, size))

        for_weight(c, go)

    def stage8(L, c):
        l = L["l"]

        for d in range(2):
            wait(o2.at[0, 0], ag_sem.at[c, l, 4 + d])

        def go(i, k):
            for d in range(2):
                there = block(wholes[i], L, L["ps"][1 - d], every, k, 1 - d)
                send(there, there, send_sem.at[c, l, 3], ag_sem.at[c, l, 6 + d], L["first"][d])

        pl.when(c < body)(lambda: for_weight(c, go))

    def stage9(L, c):
        l = L["l"]

        @pl.when(c < body)
        def _():
            for d in range(2):
                wait(o1.at[0, 0, 0], ag_sem.at[c, l, 6 + d])

    stages = (stage1, stage2, stage3, stage4, stage5, stage6, stage7, stage8, stage9)

    @pl.loop(0, chunks + STAGES - 1)
    def _(t):
        for s, stage in enumerate(stages):
            c = t - s

            @pl.when((c >= 0) & (c < chunks))
            def _():
                for L in layers:
                    stage(L, c)

    for L in layers:
        for c in (chunks - 2, chunks - 1):
            wait(m_io.at[c % 2, L["l"]], out_sem.at[c % 2, L["l"], 0])
            wait(v_io.at[c % 2, L["l"]], out_sem.at[c % 2, L["l"], 1])

    three, row, col = pl.ds(0, 3), pl.ds(0, rows), pl.ds(0, cols)

    @pl.loop(0, chunks)
    def _(c):
        for l in range(2):
            wait(wholes[0].at[l, three, every, row, col], send_sem.at[c, l, 0])
            wait(wholes[0].at[l, 0, three, row, col], send_sem.at[c, l, 1])
            wait(wholes[0].at[l, 0, three, row, col], send_sem.at[c, l, 2])
            pl.when(c < body)(lambda: wait(wholes[0].at[l, three, every, row, col], send_sem.at[c, l, 3]))
            pl.when(c >= body)(lambda: wait(wholes[0].at[l, pl.ds(0, 2), every, row, col], send_sem.at[c, l, 3]))


def stream(copies, buffer, in_sem, out_sem, ahead):
    slots = buffer.shape[0]

    def slot_of(i):
        return buffer.at[(i % slots, *(pl.ds(0, n) for n in copies[i][0].shape))]

    loads = [pltpu.make_async_copy(src, slot_of(i), in_sem.at[i % slots]) for i, (src, _) in enumerate(copies)]
    stores = [pltpu.make_async_copy(slot_of(i), dst, out_sem.at[i % slots]) for i, (_, dst) in enumerate(copies)]
    for i in range(len(copies) + ahead):
        if i < len(copies):
            if i >= slots:
                stores[i - slots].wait()
            loads[i].start()
        if i >= ahead:
            loads[i - ahead].wait()
            stores[i - ahead].start()
        yield (i + 1) / (len(copies) + ahead)
    for one in stores[-slots:]:
        one.wait()
    yield 2.0


def together(*streams):
    done = [0.0] * len(streams)
    while min(done) < 2.0:
        i = done.index(min(done))
        done[i] = next(streams[i])


def places(side):
    me = lax.axis_index("dp")
    x, y = me // side, me % side
    return [dict(l=0, p=x), dict(l=1, p=y)]


def place_in_tail(at):
    j = 0
    while at >= TAILS[j]:
        at -= TAILS[j]
        j += 1
    return j, at


def deliver_kernel(side, piece, per_weight, *refs):
    n_w = 3
    n_on = 4 * len(TAILS)
    wholes, onward, moments = refs[:n_w], refs[n_w : n_w + n_on], refs[n_w + n_on : 3 * n_w + n_on]
    refs = refs[3 * n_w + n_on :]
    outs, new_moments = refs[:n_w], refs[n_w : 3 * n_w]
    buffer, moment_buffer, in_sem, out_sem, m_in_sem, m_out_sem = refs[3 * n_w + n_on - 4 :]
    chunks = n_w * per_weight
    body = chunks - TAIL
    every = pl.ds(0, side)
    copies = []
    for c in range(chunks):
        i, k = divmod(c, per_weight)
        for L in places(side):
            for away in range(side):
                p = (L["p"] + away) % side
                parts = [block_of(piece, ref, L, p, every, k) for ref in (wholes[i], outs[i])]
                if c < body or away == 0:
                    copies.append(parts)
                elif away != 2:
                    d = 0 if away == side - 1 else 1
                    copies.append([block_of(piece, ref, L, p, every, k, d) for ref in (wholes[i], outs[i])])
                    j, at = place_in_tail(c - body)
                    copies.append([onward[4 * j + 2 * L["l"] + d].at[at], block_of(piece, outs[i], L, p, every, k, 1 - d)])
    more = []
    for old, new in zip(moments, new_moments):
        for l in range(old.shape[0]):
            for k in range(per_weight):
                more.append([ref.at[(l, *region(piece, ref, k))] for ref in (old, new)])
    together(
        stream(copies, buffer, in_sem, out_sem, buffer.shape[0] // 2),
        stream(more, moment_buffer, m_in_sem, m_out_sem, moment_buffer.shape[0] // 2),
    )


def finish_kernel(side, piece, per_weight, which, *refs):
    n_w = 3
    brought, outs, sem = refs[n_w : n_w + 4], refs[n_w + 4 : 2 * n_w + 4], refs[2 * n_w + 4]
    copies = []
    for c in range(n_w * per_weight - TAIL, n_w * per_weight):
        i, k = divmod(c, per_weight)
        j, at = place_in_tail(c - n_w * per_weight + TAIL)
        if j == which:
            for L in places(side):
                for d in range(2):
                    there = block_of(piece, outs[i], L, (L["p"] + 2) % side, pl.ds(0, side), k, 1 - d)
                    copies.append(pltpu.make_async_copy(brought[2 * L["l"] + d].at[at], there, sem.at[len(copies)]))
    for one in copies:
        one.start()
    for one in copies:
        one.wait()


def solution(mesh):
    n = mesh.shape["dp"]
    side = math.isqrt(n)

    def step(*arrays):
        terms, weights, m, v = (arrays[i : i + 3] for i in (0, 3, 6, 9))
        layers = m[0].shape[0]
        rows, cols = piece = min(one.shape[1] for one in m), min(one.shape[2] for one in m)
        sizes = {one.shape[1] * one.shape[2] for one in m}
        assert side * side == n and side == 4 and layers == 2 and len(sizes) == 1
        per_weight = sizes.pop() // (rows * cols)
        chunks = 3 * per_weight

        def blocks(a, one):
            return a.reshape(layers, side, side, *one.shape[1:])

        inputs = [blocks(a, one) for a, one in zip(terms, m)] + [blocks(a, one) for a, one in zip(weights, m)] + [*m, *v]
        outs = [jax.ShapeDtypeStruct((layers, side, side, *one.shape[1:]), BF16) for one in m]
        moments = [jax.ShapeDtypeStruct(one.shape, F32) for one in (*m, *v)]
        half = cols // 2
        onward = [jax.ShapeDtypeStruct((size, side, rows, half), BF16) for size in TAILS for _ in range(4)]
        dma = pltpu.SemaphoreType.DMA
        any_space = pl.BlockSpec(memory_space=pl.ANY)
        results = pl.pallas_call(
            functools.partial(step_kernel, side, piece, per_weight),
            out_shape=outs + moments + onward,
            in_specs=[any_space] * 12,
            out_specs=[any_space] * (9 + len(onward)),
            scratch_shapes=[
                pltpu.VMEM((chunks, layers, 2, side, rows, half), BF16),
                pltpu.VMEM((chunks, layers, 2, side, rows, cols), BF16),
                pltpu.VMEM((chunks, layers, 2, rows, half), BF16),
                pltpu.VMEM((chunks, layers, 2, rows, cols), BF16),
                pltpu.VMEM((2, layers, 2, side, rows, half), BF16),
                pltpu.VMEM((2, layers, side, rows, cols), BF16),
                pltpu.VMEM((2, layers, rows, cols), BF16),
                pltpu.VMEM((2, layers, rows, cols), F32),
                pltpu.VMEM((2, layers, rows, cols), F32),
                pltpu.VMEM((3, layers, rows, cols), F32),
                pltpu.VMEM((3, layers, 2, rows, half), F32),
                pltpu.VMEM((chunks, layers, rows, cols), BF16),
                dma((chunks, layers, 4)),
                dma((chunks, layers, 4)),
                dma((chunks, layers, 8)),
                dma((2, layers, 2)),
                dma((2, layers)),
                dma((2, layers, 3)),
                dma((2, layers, 2)),
                dma((3, layers)),
            ],
            compiler_params=pltpu.CompilerParams(collective_id=0, has_side_effects=True, vmem_limit_bytes=63 * 2**20),
            name="step",
        )(*inputs)
        wholes, moments, onward = results[:3], results[3:9], results[9:]
        hops = [
            [(x * side + y, ((x + dx) % side) * side + (y + dy) % side) for x in range(side) for y in range(side)]
            for dx, dy in ((1, 0), (-1, 0), (0, 1), (0, -1))
        ]
        brought = [lax.ppermute(one, "dp", hop) for one, hop in zip(onward[:4], hops)]
        delivered = pl.pallas_call(
            functools.partial(deliver_kernel, side, piece, per_weight),
            out_shape=outs + [jax.ShapeDtypeStruct(one.shape, one.dtype) for one in (*moments, *onward[4:])],
            in_specs=[any_space] * (9 + len(onward)),
            out_specs=[any_space] * (5 + len(onward)),
            input_output_aliases={7 + i: 9 + i for i in range(len(onward) - 4)},
            scratch_shapes=[
                pltpu.VMEM((32, side, rows, cols), BF16),
                pltpu.VMEM((32, rows, cols), F32),
                *[dma((32,))] * 4,
            ],
            compiler_params=pltpu.CompilerParams(vmem_limit_bytes=VMEM - 8 * TAILS[0] * side * rows * half - 2**17),
            cost_estimate=pl.CostEstimate(flops=10**9, bytes_accessed=10**8, transcendentals=0),
            name="deliver",
        )(*wholes, *onward, *moments)
        brought += [lax.ppermute(one, "dp", hop) for one, hop in zip(delivered[9:], hops * (len(TAILS) - 1))]
        whole = delivered[:3]
        for j, size in enumerate(TAILS):
            whole = pl.pallas_call(
                functools.partial(finish_kernel, side, piece, per_weight, j),
                out_shape=outs,
                in_specs=[any_space] * 3 + [pl.BlockSpec(memory_space=pltpu.VMEM)] * 4,
                out_specs=[any_space] * 3,
                input_output_aliases={0: 0, 1: 1, 2: 2},
                scratch_shapes=[dma((4 * size,))],
                compiler_params=pltpu.CompilerParams(vmem_limit_bytes=16 * 2**20),
                name="finish",
            )(*whole, *brought[4 * j : 4 * j + 4])
        whole = [r.reshape(a.shape) for r, a in zip(whole, weights)]
        return (*whole, *delivered[3:9])

    all_of, cut = P(None, None, None), P(None, "dp", None)
    return jax.shard_map(
        step,
        mesh=mesh,
        in_specs=(P(("rep", "dp"), None, None, None),) * 3 + (all_of,) * 3 + (cut,) * 6,
        out_specs=(P("rep", None, None),) * 3 + (P("rep", "dp", None),) * 6,
        check_vma=False,
    )
```
